256 devices in a mesh: batch: 64 (over z, y, core), group: 4 (over x).
Axes of the slice: x: 4, y: 4, z: 8, core: 2. Of those that a mesh axis runs over, the one named last changes fastest.
Arguments:
- samples_in: float32 [16384, 8192], P('batch', 'group'), may hold values from -8 to 8, as said below
- second_samples_in: float32 [16384, 8192], P('batch', 'group'), may hold values from -8 to 8, as said below
Outputs:
- standard: float32 [16384, 8192], P(None, ('group', 'batch'))
- second_standard: float32 [16384, 8192], P(None, ('group', 'batch'))
The draws below stay inside these ranges and needn't reach their ends.
Inputs may be any that keep to these rules, and one draw needn't show every extreme that they name: samples_in holds numbers from -8 to 8. second_samples_in holds numbers from -8 to 8.
All inputs are finite; a program needn't handle non-finite values.
Results may differ from the reference program's by a relative error of at most 0.0003.
Values sent between devices are 32-bit elements.
A program may use at most 64 MiB of HBM per device.

```python
import jax
import jax.numpy as jnp

ROW_DEV = 256
ROWS = 16384
COLS = 8192
N_BATCH = 64


def column_values(key, tag):
    keys = jax.random.split(jax.random.fold_in(key, tag), 4)
    level = jax.random.normal(keys[0], (1, 1, COLS), jnp.float32) * 1.0
    spread = jnp.exp(jax.random.uniform(keys[1], (1, 1, COLS), jnp.float32, -0.7, 0.7))
    drift = jax.random.normal(keys[2], (N_BATCH, 1, COLS), jnp.float32) * 1.0
    noise = jax.random.normal(keys[3], (N_BATCH, ROW_DEV, COLS), jnp.float32) * 0.6
    return level + spread * (drift + noise)


def draw_samples_in(key, part):
    values = column_values(key, 1)
    return jnp.clip(values, -8.0, 8.0).reshape(ROWS, COLS)


def draw_second_samples_in(key, part):
    values = column_values(key, 2)
    return jnp.clip(values, -8.0, 8.0).reshape(ROWS, COLS)


def setup_inputs(seed: int = 0) -> dict:
    key_list = jax.random.split(jax.random.key(seed), 3)
    return {
        "samples_in": draw_samples_in(jax.random.fold_in(key_list[2], 71), 0),
        "second_samples_in": draw_second_samples_in(jax.random.fold_in(key_list[2], 71), 0),
    }


def reference(samples_in, second_samples_in):
    wide_standard = samples_in.astype(jnp.float32)
    low_standard = jnp.mean(jnp.minimum(wide_standard, 1.0), axis=0)
    high_standard = jnp.mean(jnp.maximum(wide_standard, 1.0), axis=0)
    standard = ((wide_standard - low_standard) / (high_standard - low_standard + 0.1))
    wide_second_standard = second_samples_in.astype(jnp.float32)
    low_second_standard = jnp.mean(jnp.minimum(wide_second_standard, 1.0), axis=0)
    high_second_standard = jnp.mean(jnp.maximum(wide_second_standard, 1.0), axis=0)
    second_standard = ((wide_second_standard - low_second_standard) / (high_second_standard - low_second_standard + 0.1))
    return standard, second_standard
```

```python
import functools

import jax
import jax.numpy as jnp
from jax import lax
from jax.experimental import pallas as pl
from jax.experimental.pallas import tpu as pltpu
from jax.sharding import PartitionSpec as P

MESH = pl.DeviceIdType.MESH
LANES = 128
PLANES = 8
PER = 8
HALF = 4


def kernel(first_hbm, second_hbm, got, total, raw, turned, load_sem, send_sem, recv_sem, here, open_sem):
    n = PLANES * PER
    ins = (first_hbm, second_hbm)
    rows, width = first_hbm.shape
    block = width // n
    chunk = PER * block
    near = HALF * PER
    me = lax.axis_index("batch")
    z, y, c = me // PER, (me % PER) // 2, me % 2
    early = z < HALF

    def plane(k):
        return (z + k) % HALF + HALF * (k // HALF)

    def load(k, a):
        start = pl.multiple_of(plane(k) * chunk, chunk)
        return pltpu.make_async_copy(ins[a].at[:, pl.ds(start, chunk)], raw.at[k, a], load_sem.at[k, a])

    for k in range(PLANES):
        for a in range(2):
            load(k, a).start()

    barrier = pltpu.get_barrier_semaphore()

    def greet(target, carry):
        @pl.when(target != me)
        def _():
            pl.semaphore_signal(barrier, inc=1, device_id={"batch": target}, device_id_type=MESH)

        return carry

    @pl.when(early)
    def _():
        lax.fori_loop(0, n, greet, 0)

    def announce(target, carry):
        pl.semaphore_signal(here.at[me], inc=1, device_id={"batch": target}, device_id_type=MESH)
        return carry

    @pl.when(jnp.logical_not(early))
    def _():
        pl.semaphore_wait(barrier, near)
        lax.fori_loop(0, near, announce, 0)

    def transpose(k):
        for a in range(2):
            load(k, a).wait()
            for start in range(0, chunk, LANES):
                tile = raw[k, a, :, start : start + LANES].T
                spot = start // block
                turned[k, spot : spot + LANES // block, a] = tile.reshape(LANES // block, block, rows)

    def send(k, q, target):
        return pltpu.make_async_remote_copy(
            src_ref=turned.at[k, q],
            dst_ref=got.at[me],
            send_sem=send_sem.at[target],
            recv_sem=recv_sem.at[me],
            device_id={"batch": target},
            device_id_type=MESH,
        )

    def spot(step, first):
        k = first + step % HALF
        turn = step // HALF
        q = (y + turn // 2 + k + 2 * c) % 4 * 2 + (c + turn) % 2
        return k, q, plane(k) * PER + q

    def push_early(step, carry):
        k, q, target = spot(step, 0)

        @pl.when(target != me)
        def _():
            send(k, q, target).start()

        return carry

    def push_late(step, carry):
        k, q, target = spot(step, HALF)

        @pl.when(target != me)
        def _():
            @pl.when(early)
            def _():
                pl.semaphore_wait(here.at[target], 1)

            send(k, q, target).start()

        return carry

    for k in range(HALF):
        transpose(k)

    @pl.when(early)
    def _():
        pl.semaphore_wait(barrier, near - 1)

    lax.fori_loop(0, near, push_early, 0)
    for k in range(HALF, PLANES):
        transpose(k)

    @pl.when(jnp.logical_not(early))
    def _():
        pl.semaphore_wait(open_sem, 1)

    lax.fori_loop(0, near, push_late, 0)

    @pl.when(early)
    def _():
        pl.semaphore_signal(
            open_sem, inc=1, device_id={"batch": (PLANES - 1 - z) * PER + me % PER}, device_id_type=MESH
        )

    own = z // HALF * HALF
    got[me] = turned[own, me % PER]

    def add(sums, values):
        low, high = sums
        for start in range(0, rows, LANES):
            part = values[:, start : start + LANES]
            low += jnp.minimum(part, 1.0)
            high += jnp.maximum(part, 1.0)
        return low, high

    def take(source, sums):
        @pl.when(source != me)
        def _():
            pltpu.make_async_remote_copy(
                src_ref=turned.at[0, 0],
                dst_ref=got.at[source],
                send_sem=send_sem.at[source],
                recv_sem=recv_sem.at[source],
                device_id={"batch": source},
                device_id_type=MESH,
            ).wait_recv()

        return tuple(add(sums[a], got[source, a]) for a in range(2))

    zero = jnp.zeros((block, LANES), jnp.float32)
    sums = lax.fori_loop(0, n, take, ((zero, zero), (zero, zero)))
    for a in range(2):
        for kind in range(2):
            total[a, kind] = sums[a][kind]

    def drain(step, carry):
        k, q, target = spot(step % near, step // near * HALF)

        @pl.when(target != me)
        def _():
            send(k, q, target).wait_send()

        return carry

    lax.fori_loop(0, n, drain, 0)


def rescale(got, total, first_out, second_out, ready, store_sem):
    n, _, block, rows = got.shape
    outs = (first_out, second_out)
    pieces = 4
    each = n // pieces
    copies = []
    for a in range(2):
        low, high = (
            jnp.sum(total[a, kind], axis=1, keepdims=True) / (n * rows) for kind in range(2)
        )
        scale = 1.0 / (high - low + 0.1)
        low = jnp.broadcast_to(low, (block, rows))
        scale = jnp.broadcast_to(scale, (block, rows))
        for piece in range(pieces):

            def turn(step, carry, a=a, piece=piece, low=low, scale=scale):
                source = piece * each + step
                start = pl.multiple_of(source * rows, LANES)
                ready[a, :, pl.ds(start, rows)] = (got[source, a] - low) * scale
                return carry

            lax.fori_loop(0, each, turn, 0)
            part = pl.ds(piece * each * rows, each * rows)
            copy = pltpu.make_async_copy(
                ready.at[a, :, part], outs[a].at[:, part], store_sem.at[a, piece]
            )
            copy.start()
            copies.append(copy)
    for copy in copies:
        copy.wait()


def solution(mesh):
    n = mesh.shape["batch"]

    def shards(samples_in, second_samples_in):
        rows, width = samples_in.shape
        block = width // n
        held = 2 * rows * width * 4
        got, total = pl.pallas_call(
            kernel,
            out_shape=(
                pltpu.VMEM((n, 2, block, rows), jnp.float32),
                pltpu.VMEM((2, 2, block, LANES), jnp.float32),
            ),
            in_specs=[pl.BlockSpec(memory_space=pltpu.HBM)] * 2,
            out_specs=[pl.BlockSpec(memory_space=pltpu.VMEM)] * 2,
            scratch_shapes=[
                pltpu.VMEM((PLANES, 2, rows, PER * block), jnp.float32),
                pltpu.VMEM((PLANES, PER, 2, block, rows), jnp.float32),
                pltpu.SemaphoreType.DMA((PLANES, 2)),
                pltpu.SemaphoreType.DMA((n,)),
                pltpu.SemaphoreType.DMA((n,)),
                pltpu.SemaphoreType.REGULAR((n,)),
                pltpu.SemaphoreType.REGULAR,
            ],
            compiler_params=pltpu.CompilerParams(
                collective_id=0, has_side_effects=True, vmem_limit_bytes=4 * held + (8 << 20)
            ),
            name="exchange",
        )(
            pltpu.with_memory_space_constraint(samples_in, pltpu.HBM),
            pltpu.with_memory_space_constraint(second_samples_in, pltpu.HBM),
        )
        out = jax.ShapeDtypeStruct((block, n * rows), jnp.float32)
        first, second = pl.pallas_call(
            rescale,
            out_shape=(out, out),
            in_specs=[pl.BlockSpec(memory_space=pltpu.VMEM)] * 2,
            out_specs=[pl.BlockSpec(memory_space=pl.ANY)] * 2,
            scratch_shapes=[
                pltpu.VMEM((2, block, n * rows), jnp.float32),
                pltpu.SemaphoreType.DMA((2, 4)),
            ],
            compiler_params=pltpu.CompilerParams(vmem_limit_bytes=2 * held + (8 << 20)),
            name="rescale",
        )(
            pltpu.with_memory_space_constraint(got, pltpu.VMEM),
            pltpu.with_memory_space_constraint(total, pltpu.VMEM),
        )
        return first.T, second.T

    placed = (P("batch", "group"), P("batch", "group"))
    return jax.shard_map(
        shards,
        mesh=mesh,
        in_specs=placed,
        out_specs=(P(None, ("group", "batch")), P(None, ("group", "batch"))),
        check_vma=False,
    )
```

```python
import functools

import jax
import jax.numpy as jnp
from jax import lax
from jax.experimental import pallas as pl
from jax.experimental.pallas import tpu as pltpu
from jax.sharding import PartitionSpec as P

MESH = pl.DeviceIdType.MESH
LANES = 128
PLANES = 8
PER = 8
ORDER = (4, 3, 5, 2, 6, 1, 7, 0)
SHIFT = (0, 0, 1, 0, 1, 0, 1, 0)
LOADS = (1, 7, 4, 3, 5, 2, 6, 0)
FIRST = 3
PHASES = (('F', 0, 3), ('A', 3, 8))
STEPS = sum(d * 8**i for i, d in enumerate(ORDER))
TURNS = sum(d * 4**i for i, d in enumerate(SHIFT))
NEAR = sum((d in (1, PLANES - 1)) << i for i, d in enumerate(ORDER))
OWN = ORDER.index(0)


def at(table, bits, i):
    return lax.shift_right_logical(jnp.int32(table), bits * i) % 2**bits


def kernel(first_hbm, second_hbm, got, total, raw, turned, load_sem, send_sem, recv_sem, here):
    n = PLANES * PER
    ins = (first_hbm, second_hbm)
    rows, width = first_hbm.shape
    block = width // n
    chunk = PER * block
    me = lax.axis_index("batch")
    z, y, c = me // PER, (me % PER) // 2, me % 2

    def plane(k):
        return (z + LOADS[k]) % PLANES

    for k in range(PLANES):
        for a in range(2):
            start = pl.multiple_of(plane(k) * chunk, chunk)
            pltpu.make_async_copy(
                ins[a].at[:, pl.ds(start, chunk)], raw.at[k, a], load_sem.at[k]
            ).start()

    barrier = pltpu.get_barrier_semaphore()

    def greet(step, carry):
        side = step // PER * (PLANES - 2) + 1
        target = (z + side) % PLANES * PER + (me + step) % PER
        pl.semaphore_signal(barrier, inc=1, device_id={"batch": target}, device_id_type=MESH)
        return carry

    lax.fori_loop(0, 2 * PER, greet, 0)

    def hail(which, dz):
        for slot, d in ((0, dz), (1, PLANES - dz)):
            target = (z + d) % PLANES * PER + me % PER
            pl.semaphore_signal(
                here.at[which, slot], inc=1, device_id={"batch": target}, device_id_type=MESH
            )

    def heard(which):
        for slot in range(2):
            pl.semaphore_wait(here.at[which, slot], 1)

    def transpose(k):
        pltpu.make_async_copy(raw.at[k], raw.at[k], load_sem.at[k]).wait()
        for a in range(2):
            for start in range(0, chunk, LANES):
                tile = raw[k, a, :, start : start + LANES].T
                spot = plane(k) * PER + start // block
                turned[pl.ds(spot, LANES // block), a] = tile.reshape(LANES // block, block, rows)

    def push(mask, r0, r1):
        def one(step, carry):
            i = step % PLANES
            turn = step // PLANES
            zt = (z + at(STEPS, 3, i)) % PLANES
            target = zt * PER + (y + turn // 2 + at(TURNS, 2, i) + 2 * c) % 4 * 2 + (c + turn) % 2
            ok = target != me
            if mask != "A":
                ok = ok & (at(NEAR, 1, i) == (1 if mask == "N" else 0))

            @pl.when(ok)
            def _():
                pltpu.make_async_remote_copy(
                    src_ref=turned.at[target],
                    dst_ref=got.at[me],
                    send_sem=send_sem,
                    recv_sem=recv_sem.at[turn],
                    device_id={"batch": target},
                    device_id_type=MESH,
                ).start()

            return carry

        lax.fori_loop(r0 * PLANES, r1 * PLANES, one, 0)

    for k in range(2):
        transpose(k)
    pl.semaphore_wait(barrier, 2 * PER)
    hail(0, 1)
    push("N", 0, FIRST)
    for k in range(2, 5):
        transpose(k)
    heard(0)
    hail(1, 2)
    for k in range(5, PLANES):
        transpose(k)
    heard(1)
    for mask, r0, r1 in PHASES:
        push(mask, r0, r1)

    got[me] = turned[me]

    def arrived(count, turn):
        pieces = pl.ds(0, count)
        pltpu.make_async_remote_copy(
            src_ref=turned.at[pieces],
            dst_ref=got.at[pieces],
            send_sem=send_sem,
            recv_sem=recv_sem.at[turn],
            device_id={"batch": (me + 1) % n},
            device_id_type=MESH,
        ).wait_recv()

    def take(turn, sums):
        own = turn == (8 - SHIFT[OWN] - 2 * c) % 4 * 2

        @pl.when(own)
        def _():
            arrived(PLANES - 1, turn)

        @pl.when(jnp.logical_not(own))
        def _():
            arrived(PLANES, turn)

        def add(i, sums):
            cs = (c + turn) % 2
            ys = (y - turn // 2 - at(TURNS, 2, i) - 2 * cs + 16) % 4
            source = (z - at(STEPS, 3, i) + PLANES) % PLANES * PER + ys * 2 + cs
            out = []
            for a in range(2):
                low, high = sums[a]
                values = got[source, a]
                for start in range(0, rows, LANES):
                    part = values[:, start : start + LANES]
                    low += jnp.minimum(part, 1.0)
                    high += jnp.maximum(part, 1.0)
                out.append((low, high))
            return tuple(out)

        return lax.fori_loop(0, PLANES, add, sums)

    zero = jnp.zeros((block, LANES), jnp.float32)
    sums = lax.fori_loop(0, PER, take, ((zero, zero), (zero, zero)))
    for a in range(2):
        for kind in range(2):
            total[a, kind] = sums[a][kind]

    others = pl.ds(0, n - 1)
    pltpu.make_async_remote_copy(
        src_ref=turned.at[others],
        dst_ref=got.at[others],
        send_sem=send_sem,
        recv_sem=recv_sem.at[0],
        device_id={"batch": (me + 1) % n},
        device_id_type=MESH,
    ).wait_send()


def rescale(got, total, first_out, second_out, ready, store_sem):
    n, _, block, rows = got.shape
    outs = (first_out, second_out)
    pieces = 4
    each = n // pieces
    copies = []
    for a in range(2):
        low, high = (
            jnp.sum(total[a, kind], axis=1, keepdims=True) / (n * rows) for kind in range(2)
        )
        scale = 1.0 / (high - low + 0.1)
        low = jnp.broadcast_to(low, (block, rows))
        scale = jnp.broadcast_to(scale, (block, rows))
        for piece in range(pieces):

            def turn(step, carry, a=a, piece=piece, low=low, scale=scale):
                source = piece * each + step
                start = pl.multiple_of(source * rows, LANES)
                ready[a, :, pl.ds(start, rows)] = (got[source, a] - low) * scale
                return carry

            lax.fori_loop(0, each, turn, 0, unroll=4)
            part = pl.ds(piece * each * rows, each * rows)
            copy = pltpu.make_async_copy(
                ready.at[a, :, part], outs[a].at[:, part], store_sem.at[a, piece]
            )
            copy.start()
            copies.append(copy)
    for copy in copies:
        copy.wait()


def solution(mesh):
    n = mesh.shape["batch"]

    def shards(samples_in, second_samples_in):
        rows, width = samples_in.shape
        block = width // n
        held = 2 * rows * width * 4
        got, total = pl.pallas_call(
            kernel,
            out_shape=(
                pltpu.VMEM((n, 2, block, rows), jnp.float32),
                pltpu.VMEM((2, 2, block, LANES), jnp.float32),
            ),
            in_specs=[pl.BlockSpec(memory_space=pltpu.HBM)] * 2,
            out_specs=[pl.BlockSpec(memory_space=pltpu.VMEM)] * 2,
            scratch_shapes=[
                pltpu.VMEM((PLANES, 2, rows, PER * block), jnp.float32),
                pltpu.VMEM((n, 2, block, rows), jnp.float32),
                pltpu.SemaphoreType.DMA((PLANES,)),
                pltpu.SemaphoreType.DMA,
                pltpu.SemaphoreType.DMA((PER,)),
                pltpu.SemaphoreType.REGULAR((2, 2)),
            ],
            compiler_params=pltpu.CompilerParams(
                collective_id=0, has_side_effects=True, vmem_limit_bytes=4 * held + (8 << 20)
            ),
            name="exchange",
        )(
            pltpu.with_memory_space_constraint(samples_in, pltpu.HBM),
            pltpu.with_memory_space_constraint(second_samples_in, pltpu.HBM),
        )
        out = jax.ShapeDtypeStruct((block, n * rows), jnp.float32)
        first, second = pl.pallas_call(
            rescale,
            out_shape=(out, out),
            in_specs=[pl.BlockSpec(memory_space=pltpu.VMEM)] * 2,
            out_specs=[pl.BlockSpec(memory_space=pl.ANY)] * 2,
            scratch_shapes=[
                pltpu.VMEM((2, block, n * rows), jnp.float32),
                pltpu.SemaphoreType.DMA((2, 4)),
            ],
            compiler_params=pltpu.CompilerParams(vmem_limit_bytes=2 * held + (8 << 20)),
            name="rescale",
        )(
            pltpu.with_memory_space_constraint(got, pltpu.VMEM),
            pltpu.with_memory_space_constraint(total, pltpu.VMEM),
        )
        return first.T, second.T

    placed = (P("batch", "group"), P("batch", "group"))
    return jax.shard_map(
        shards,
        mesh=mesh,
        in_specs=placed,
        out_specs=(P(None, ("group", "batch")), P(None, ("group", "batch"))),
        check_vma=False,
    )
```

```python
import functools

import jax
import jax.numpy as jnp
from jax import lax
from jax.experimental import pallas as pl
from jax.experimental.pallas import tpu as pltpu
from jax.sharding import PartitionSpec as P

MESH = pl.DeviceIdType.MESH
LANES = 128
PLANES = 8
PER = 8
ORDER = (4, 3, 5, 2, 6, 1, 7, 0)
SHIFT = (0, 0, 1, 0, 1, 0, 1, 0)
LOADS = (1, 7, 4, 3, 5, 2, 6, 0)
FIRST = 4
PHASES = (('F', 0, 4), ('A', 4, 6), ('O', 6, 8), ('L', 6, 8), ('H', 6, 8))
EARLY = 4
NEAR = (1, PLANES - 1)
OWN = ORDER.index(0)
BESIDE = ((1, 2, 3), (3, 1, 2), (2, 3, 1), (1, 3, 2))


def along(i, turn, core):
    j = turn // 2
    if ORDER[i] not in NEAR:
        return (j + SHIFT[i] + 2 * core) % 4
    one, two = (
        sum(d * 4 ** (k + 1) for k, d in enumerate(BESIDE[NEAR.index(ORDER[i]) * 2 + side])) for side in range(2)
    )
    return lax.shift_right_logical(jnp.where(core == 0, one, two), 2 * j) % 4


def kernel(first_hbm, second_hbm, got, total, raw, turned, load_sem, send_sem, recv_sem, here):
    n = PLANES * PER
    ins = (first_hbm, second_hbm)
    rows, width = first_hbm.shape
    block = width // n
    chunk = PER * block
    me = lax.axis_index("batch")
    z, y, c = me // PER, (me % PER) // 2, me % 2

    def plane(k):
        return (z + LOADS[k]) % PLANES

    def load(k):
        for a in range(2):
            start = pl.multiple_of(plane(k) * chunk, chunk)
            pltpu.make_async_copy(
                ins[a].at[:, pl.ds(start, chunk)], raw.at[k, a], load_sem.at[k]
            ).start()

    for k in range(2):
        load(k)

    barrier = pltpu.get_barrier_semaphore()

    def device(dz, dy, dc=0):
        return (z + dz) % PLANES * PER + (y + dy) % 4 * 2 + (c + dc) % 2

    def signal(sem, target):
        pl.semaphore_signal(sem, inc=1, device_id={"batch": target}, device_id_type=MESH)

    for dz in (1, PLANES - 1):
        for dc in range(2):
            signal(barrier, device(dz, 0, dc))
    for dy in range(1, 4):
        signal(barrier, device(0, dy))
    for k in range(2, PLANES):
        load(k)

    def hail(which, dz):
        for slot, d in ((0, dz), (1, PLANES - dz)):
            signal(here.at[which, slot], device(d, 0))

    def heard(which, slots):
        for slot in range(slots):
            pl.semaphore_wait(here.at[which, slot], 1)

    def transpose(k):
        pltpu.make_async_copy(raw.at[k], raw.at[k], load_sem.at[k]).wait()
        for a in range(2):
            for start in range(0, chunk, LANES):
                tile = raw[k, a, :, start : start + LANES].T
                spot = plane(k) * PER + start // block
                turned[pl.ds(spot, LANES // block), a] = tile.reshape(LANES // block, block, rows)

    def send(i, turn, wanted=None):
        zt = (z + ORDER[i]) % PLANES
        yt = (y + along(i, turn, c)) % 4
        target = zt * PER + yt * 2 + (c + turn) % 2

        def go():
            pltpu.make_async_remote_copy(
                src_ref=turned.at[target],
                dst_ref=got.at[me],
                send_sem=send_sem,
                recv_sem=recv_sem.at[turn],
                device_id={"batch": target},
                device_id_type=MESH,
            ).start()

        ok = wanted(zt, yt) if wanted else None
        if ORDER[i] == 0:
            ok = target != me if ok is None else ok & (target != me)
        if ok is None:
            go()
        else:
            pl.when(ok)(go)

    WANTED = {
        "O": lambda zt, yt: (zt == 0),
        "L": lambda zt, yt: (zt < EARLY) & jnp.logical_not((zt == 0)),
        "l": lambda zt, yt: zt < EARLY,
        "H": lambda zt, yt: zt >= EARLY,
    }

    def push(mask, r0, r1):
        which = [i for i in range(PLANES) if not (mask == "N" and ORDER[i] not in NEAR or mask == "F" and ORDER[i] in NEAR)]

        def one(turn, carry):
            for i in which:
                send(i, turn, WANTED.get(mask))
            return carry

        if r1 - r0 <= 2 and mask in "N":
            for turn in range(r0, r1):
                one(turn, 0)
        else:
            lax.fori_loop(r0, r1, one, 0)

    def pair(dz):
        for turn in range(2):
            send(ORDER.index(dz), turn)

    transpose(0)
    pl.semaphore_wait(barrier, 7)
    for dy in range(1, 4):
        signal(here.at[0, dy - 1], device(0, dy))
    pair(1)
    transpose(1)
    pair(PLANES - 1)
    for k in range(2, 4):
        transpose(k)
    heard(0, 3)
    hail(1, 1)
    push("N", 2, FIRST)
    for k in range(4, 6):
        transpose(k)
    heard(1, 2)
    hail(2, 2)
    for k in range(6, PLANES):
        transpose(k)
    heard(2, 2)
    for mask, r0, r1 in PHASES:
        push(mask, r0, r1)

    got[me] = turned[me]

    def arrived(count, turn):
        pieces = pl.ds(0, count)
        pltpu.make_async_remote_copy(
            src_ref=turned.at[pieces],
            dst_ref=got.at[pieces],
            send_sem=send_sem,
            recv_sem=recv_sem.at[turn],
            device_id={"batch": (me + 1) % n},
            device_id_type=MESH,
        ).wait_recv()

    def take(turn, sums):
        own = turn == (8 - SHIFT[OWN] - 2 * c) % 4 * 2

        @pl.when(own)
        def _():
            arrived(PLANES - 1, turn)

        @pl.when(jnp.logical_not(own))
        def _():
            arrived(PLANES, turn)

        for i in range(PLANES):
            cs = (c + turn) % 2
            ys = (y - along(i, turn, cs) + 4) % 4
            source = (z - ORDER[i] + PLANES) % PLANES * PER + ys * 2 + cs
            out = []
            for a in range(2):
                low, high = sums[a]
                values = got[source, a]
                for start in range(0, rows, LANES):
                    part = values[:, start : start + LANES]
                    low += jnp.minimum(part, 1.0)
                    high += jnp.maximum(part, 1.0)
                out.append((low, high))
            sums = tuple(out)
        return sums

    zero = jnp.zeros((block, LANES), jnp.float32)
    sums = lax.fori_loop(0, PER, take, ((zero, zero), (zero, zero)))
    for a in range(2):
        for kind in range(2):
            total[a, kind] = sums[a][kind]

    others = pl.ds(0, n - 1)
    pltpu.make_async_remote_copy(
        src_ref=turned.at[others],
        dst_ref=got.at[others],
        send_sem=send_sem,
        recv_sem=recv_sem.at[0],
        device_id={"batch": (me + 1) % n},
        device_id_type=MESH,
    ).wait_send()


def rescale(got, total, first_out, second_out, ready, store_sem):
    n, _, block, rows = got.shape
    outs = (first_out, second_out)
    pieces = 4
    each = n // pieces
    copies = []
    for a in range(2):
        low, high = (
            jnp.sum(total[a, kind], axis=1, keepdims=True) / (n * rows) for kind in range(2)
        )
        scale = 1.0 / (high - low + 0.1)
        low = jnp.broadcast_to(low, (block, rows))
        scale = jnp.broadcast_to(scale, (block, rows))
        for piece in range(pieces):

            def turn(step, carry, a=a, piece=piece, low=low, scale=scale):
                source = piece * each + step
                start = pl.multiple_of(source * rows, LANES)
                ready[a, :, pl.ds(start, rows)] = (got[source, a] - low) * scale
                return carry

            lax.fori_loop(0, each, turn, 0, unroll=4)
            part = pl.ds(piece * each * rows, each * rows)
            copy = pltpu.make_async_copy(
                ready.at[a, :, part], outs[a].at[:, part], store_sem.at[a, piece]
            )
            copy.start()
            copies.append(copy)
    for copy in copies:
        copy.wait()


def solution(mesh):
    n = mesh.shape["batch"]

    def shards(samples_in, second_samples_in):
        rows, width = samples_in.shape
        block = width // n
        held = 2 * rows * width * 4
        got, total = pl.pallas_call(
            kernel,
            out_shape=(
                pltpu.VMEM((n, 2, block, rows), jnp.float32),
                pltpu.VMEM((2, 2, block, LANES), jnp.float32),
            ),
            in_specs=[pl.BlockSpec(memory_space=pltpu.HBM)] * 2,
            out_specs=[pl.BlockSpec(memory_space=pltpu.VMEM)] * 2,
            scratch_shapes=[
                pltpu.VMEM((PLANES, 2, rows, PER * block), jnp.float32),
                pltpu.VMEM((n, 2, block, rows), jnp.float32),
                pltpu.SemaphoreType.DMA((PLANES,)),
                pltpu.SemaphoreType.DMA,
                pltpu.SemaphoreType.DMA((PER,)),
                pltpu.SemaphoreType.REGULAR((3, 3)),
            ],
            compiler_params=pltpu.CompilerParams(
                collective_id=0, has_side_effects=True, vmem_limit_bytes=4 * held + (8 << 20)
            ),
            name="exchange",
        )(
            pltpu.with_memory_space_constraint(samples_in, pltpu.HBM),
            pltpu.with_memory_space_constraint(second_samples_in, pltpu.HBM),
        )
        out = jax.ShapeDtypeStruct((block, n * rows), jnp.float32)
        first, second = pl.pallas_call(
            rescale,
            out_shape=(out, out),
            in_specs=[pl.BlockSpec(memory_space=pltpu.VMEM)] * 2,
            out_specs=[pl.BlockSpec(memory_space=pl.ANY)] * 2,
            scratch_shapes=[
                pltpu.VMEM((2, block, n * rows), jnp.float32),
                pltpu.SemaphoreType.DMA((2, 4)),
            ],
            compiler_params=pltpu.CompilerParams(vmem_limit_bytes=2 * held + (8 << 20)),
            name="rescale",
        )(
            pltpu.with_memory_space_constraint(got, pltpu.VMEM),
            pltpu.with_memory_space_constraint(total, pltpu.VMEM),
        )
        return first.T, second.T

    placed = (P("batch", "group"), P("batch", "group"))
    return jax.shard_map(
        shards,
        mesh=mesh,
        in_specs=placed,
        out_specs=(P(None, ("group", "batch")), P(None, ("group", "batch"))),
        check_vma=False,
    )
```

```python
import functools

import jax
import jax.numpy as jnp
from jax import lax
from jax.experimental import pallas as pl
from jax.experimental.pallas import tpu as pltpu
from jax.sharding import PartitionSpec as P

MESH = pl.DeviceIdType.MESH
LANES = 128
PLANES = 8
PER = 8
ORDER = (7, 3, 5, 2, 6, 1, 4, 0)
SHIFT = (1, 0, 1, 0, 1, 0, 0, 0)
LOADS = (1, 7, 4, 3, 5, 2, 6, 0)
FIRST = 4
PHASES = (('F', 0, 4), ('A', 4, 7), ('0', 7, 8), ('1', 7, 8), ('2', 7, 8), ('3', 7, 8), ('4', 7, 8))
EARLY = 4
NEAR = (1, PLANES - 1)
OWN = ORDER.index(0)
BESIDE = ((1, 2, 3), (3, 1, 2), (2, 3, 1), (1, 3, 2))


def along(i, turn, core):
    j = turn // 2
    if ORDER[i] not in NEAR:
        return (j + SHIFT[i] + 2 * core) % 4
    one, two = (
        sum(d * 4 ** (k + 1) for k, d in enumerate(BESIDE[NEAR.index(ORDER[i]) * 2 + side])) for side in range(2)
    )
    return lax.shift_right_logical(jnp.where(core == 0, one, two), 2 * j) % 4


def kernel(first_hbm, second_hbm, got, total, raw, turned, load_sem, send_sem, recv_sem, here):
    n = PLANES * PER
    ins = (first_hbm, second_hbm)
    rows, width = first_hbm.shape
    block = width // n
    chunk = PER * block
    me = lax.axis_index("batch")
    z, y, c = me // PER, (me % PER) // 2, me % 2

    def plane(k):
        return (z + LOADS[k]) % PLANES

    def load(k):
        for a in range(2):
            start = pl.multiple_of(plane(k) * chunk, chunk)
            pltpu.make_async_copy(
                ins[a].at[:, pl.ds(start, chunk)], raw.at[k, a], load_sem.at[k]
            ).start()

    for k in range(2):
        load(k)

    barrier = pltpu.get_barrier_semaphore()

    def device(dz, dy, dc=0):
        return (z + dz) % PLANES * PER + (y + dy) % 4 * 2 + (c + dc) % 2

    def signal(sem, target):
        pl.semaphore_signal(sem, inc=1, device_id={"batch": target}, device_id_type=MESH)

    for dz in (1, PLANES - 1):
        for dc in range(2):
            signal(barrier, device(dz, 0, dc))
    for dy in range(1, 4):
        signal(barrier, device(0, dy))
    for k in range(2, PLANES):
        load(k)

    def hail(which, dz):
        for slot, d in ((0, dz), (1, PLANES - dz)):
            signal(here.at[which, slot], device(d, 0))

    def heard(which, slots):
        for slot in range(slots):
            pl.semaphore_wait(here.at[which, slot], 1)

    def transpose(k):
        pltpu.make_async_copy(raw.at[k], raw.at[k], load_sem.at[k]).wait()
        for a in range(2):
            for start in range(0, chunk, LANES):
                tile = raw[k, a, :, start : start + LANES].T
                spot = plane(k) * PER + start // block
                turned[pl.ds(spot, LANES // block), a] = tile.reshape(LANES // block, block, rows)

    def send(i, turn, wanted=None):
        zt = (z + ORDER[i]) % PLANES
        yt = (y + along(i, turn, c)) % 4
        target = zt * PER + yt * 2 + (c + turn) % 2

        def go():
            pltpu.make_async_remote_copy(
                src_ref=turned.at[target],
                dst_ref=got.at[me],
                send_sem=send_sem,
                recv_sem=recv_sem.at[turn],
                device_id={"batch": target},
                device_id_type=MESH,
            ).start()

        ok = wanted(zt, yt) if wanted else None
        if ORDER[i] == 0:
            ok = target != me if ok is None else ok & (target != me)
        if ok is None:
            go()
        else:
            pl.when(ok)(go)

    def urgency(level):
        def wanted(zt, yt):
            first = jnp.minimum(z, zt)
            return first >= level if level == EARLY else first == level

        return wanted

    def push(mask, r0, r1):
        which = [i for i in range(PLANES) if not (mask == "N" and ORDER[i] not in NEAR or mask == "F" and ORDER[i] in NEAR)]

        def one(turn, carry):
            for i in which:
                send(i, turn, urgency(int(mask)) if mask.isdigit() else None)
            return carry

        if r1 - r0 <= 2 and mask in "N":
            for turn in range(r0, r1):
                one(turn, 0)
        else:
            lax.fori_loop(r0, r1, one, 0)

    def pair(dz):
        for turn in range(2):
            send(ORDER.index(dz), turn)

    transpose(0)
    pl.semaphore_wait(barrier, 7)
    for dy in range(1, 4):
        signal(here.at[0, dy - 1], device(0, dy))
    pair(1)
    transpose(1)
    pair(PLANES - 1)
    for k in range(2, 4):
        transpose(k)
    heard(0, 3)
    hail(1, 1)
    push("N", 2, FIRST)
    for k in range(4, 6):
        transpose(k)
    heard(1, 2)
    hail(2, 2)
    for k in range(6, PLANES):
        transpose(k)
    heard(2, 2)
    for mask, r0, r1 in PHASES:
        push(mask, r0, r1)

    got[me] = turned[me]

    def arrived(count, turn):
        pieces = pl.ds(0, count)
        pltpu.make_async_remote_copy(
            src_ref=turned.at[pieces],
            dst_ref=got.at[pieces],
            send_sem=send_sem,
            recv_sem=recv_sem.at[turn],
            device_id={"batch": (me + 1) % n},
            device_id_type=MESH,
        ).wait_recv()

    def take(turn, sums):
        own = turn == (8 - SHIFT[OWN] - 2 * c) % 4 * 2

        @pl.when(own)
        def _():
            arrived(PLANES - 1, turn)

        @pl.when(jnp.logical_not(own))
        def _():
            arrived(PLANES, turn)

        for i in range(PLANES):
            cs = (c + turn) % 2
            ys = (y - along(i, turn, cs) + 4) % 4
            source = (z - ORDER[i] + PLANES) % PLANES * PER + ys * 2 + cs
            out = []
            for a in range(2):
                low, high = sums[a]
                values = got[source, a]
                for start in range(0, rows, LANES):
                    part = values[:, start : start + LANES]
                    low += jnp.minimum(part, 1.0)
                    high += jnp.maximum(part, 1.0)
                out.append((low, high))
            sums = tuple(out)
        return sums

    zero = jnp.zeros((block, LANES), jnp.float32)
    sums = lax.fori_loop(0, PER, take, ((zero, zero), (zero, zero)))
    for a in range(2):
        for kind in range(2):
            total[a, kind] = sums[a][kind]

    others = pl.ds(0, n - 1)
    pltpu.make_async_remote_copy(
        src_ref=turned.at[others],
        dst_ref=got.at[others],
        send_sem=send_sem,
        recv_sem=recv_sem.at[0],
        device_id={"batch": (me + 1) % n},
        device_id_type=MESH,
    ).wait_send()


def rescale(got, total, first_out, second_out, ready, store_sem):
    n, _, block, rows = got.shape
    outs = (first_out, second_out)
    pieces = 4
    each = n // pieces
    copies = []
    for a in range(2):
        low, high = (
            jnp.sum(total[a, kind], axis=1, keepdims=True) / (n * rows) for kind in range(2)
        )
        scale = 1.0 / (high - low + 0.1)
        low = jnp.broadcast_to(low, (block, rows))
        scale = jnp.broadcast_to(scale, (block, rows))
        for piece in range(pieces):

            def turn(step, carry, a=a, piece=piece, low=low, scale=scale):
                source = piece * each + step
                start = pl.multiple_of(source * rows, LANES)
                ready[a, :, pl.ds(start, rows)] = (got[source, a] - low) * scale
                return carry

            lax.fori_loop(0, each, turn, 0, unroll=4)
            part = pl.ds(piece * each * rows, each * rows)
            copy = pltpu.make_async_copy(
                ready.at[a, :, part], outs[a].at[:, part], store_sem.at[a, piece]
            )
            copy.start()
            copies.append(copy)
    for copy in copies:
        copy.wait()


def solution(mesh):
    n = mesh.shape["batch"]

    def shards(samples_in, second_samples_in):
        rows, width = samples_in.shape
        block = width // n
        held = 2 * rows * width * 4
        got, total = pl.pallas_call(
            kernel,
            out_shape=(
                pltpu.VMEM((n, 2, block, rows), jnp.float32),
                pltpu.VMEM((2, 2, block, LANES), jnp.float32),
            ),
            in_specs=[pl.BlockSpec(memory_space=pltpu.HBM)] * 2,
            out_specs=[pl.BlockSpec(memory_space=pltpu.VMEM)] * 2,
            scratch_shapes=[
                pltpu.VMEM((PLANES, 2, rows, PER * block), jnp.float32),
                pltpu.VMEM((n, 2, block, rows), jnp.float32),
                pltpu.SemaphoreType.DMA((PLANES,)),
                pltpu.SemaphoreType.DMA,
                pltpu.SemaphoreType.DMA((PER,)),
                pltpu.SemaphoreType.REGULAR((3, 3)),
            ],
            compiler_params=pltpu.CompilerParams(
                collective_id=0, has_side_effects=True, vmem_limit_bytes=4 * held + (8 << 20)
            ),
            name="exchange",
        )(
            pltpu.with_memory_space_constraint(samples_in, pltpu.HBM),
            pltpu.with_memory_space_constraint(second_samples_in, pltpu.HBM),
        )
        out = jax.ShapeDtypeStruct((block, n * rows), jnp.float32)
        first, second = pl.pallas_call(
            rescale,
            out_shape=(out, out),
            in_specs=[pl.BlockSpec(memory_space=pltpu.VMEM)] * 2,
            out_specs=[pl.BlockSpec(memory_space=pl.ANY)] * 2,
            scratch_shapes=[
                pltpu.VMEM((2, block, n * rows), jnp.float32),
                pltpu.SemaphoreType.DMA((2, 4)),
            ],
            compiler_params=pltpu.CompilerParams(vmem_limit_bytes=2 * held + (8 << 20)),
            name="rescale",
        )(
            pltpu.with_memory_space_constraint(got, pltpu.VMEM),
            pltpu.with_memory_space_constraint(total, pltpu.VMEM),
        )
        return first.T, second.T

    placed = (P("batch", "group"), P("batch", "group"))
    return jax.shard_map(
        shards,
        mesh=mesh,
        in_specs=placed,
        out_specs=(P(None, ("group", "batch")), P(None, ("group", "batch"))),
        check_vma=False,
    )
```

```python
import functools

import jax
import jax.numpy as jnp
from jax import lax
from jax.experimental import pallas as pl
from jax.experimental.pallas import tpu as pltpu
from jax.sharding import PartitionSpec as P

MESH = pl.DeviceIdType.MESH
LANES = 128
PLANES = 8
PER = 8
ORDER = (7, 3, 5, 2, 6, 1, 4, 0)
SHIFT = (1, 0, 1, 0, 1, 0, 0, 0)
LOADS = (1, 7, 2, 6, 4, 3, 5, 0)
FIRST = 3
PHASES = (('G', 0, 2), ('F', 2, 3), ('A', 3, 7), ('0', 7, 8), ('1', 7, 8), ('2', 7, 8), ('3', 7, 8), ('4', 7, 8))
SECOND = 2
EARLY = 4
NEAR = (1, PLANES - 1)
TWO = (2, PLANES - 2)
OWN = ORDER.index(0)
BESIDE = ((1, 2, 3), (3, 1, 2), (2, 3, 1), (1, 3, 2))


def along(i, turn, core):
    j = turn // 2
    if ORDER[i] not in NEAR:
        return (j + SHIFT[i] + 2 * core) % 4
    one, two = (
        sum(d * 4 ** (k + 1) for k, d in enumerate(BESIDE[NEAR.index(ORDER[i]) * 2 + side])) for side in range(2)
    )
    return lax.shift_right_logical(jnp.where(core == 0, one, two), 2 * j) % 4


def kernel(first_hbm, second_hbm, got, total, raw, turned, load_sem, send_sem, recv_sem, here):
    n = PLANES * PER
    ins = (first_hbm, second_hbm)
    rows, width = first_hbm.shape
    block = width // n
    chunk = PER * block
    me = lax.axis_index("batch")
    z, y, c = me // PER, (me % PER) // 2, me % 2

    def plane(k):
        return (z + LOADS[k]) % PLANES

    def load(k):
        for a in range(2):
            start = pl.multiple_of(plane(k) * chunk, chunk)
            pltpu.make_async_copy(
                ins[a].at[:, pl.ds(start, chunk)], raw.at[k, a], load_sem.at[k]
            ).start()

    for k in range(2):
        load(k)

    barrier = pltpu.get_barrier_semaphore()

    def device(dz, dy, dc=0):
        return (z + dz) % PLANES * PER + (y + dy) % 4 * 2 + (c + dc) % 2

    def signal(sem, target):
        pl.semaphore_signal(sem, inc=1, device_id={"batch": target}, device_id_type=MESH)

    for dz in (1, PLANES - 1):
        for dc in range(2):
            signal(barrier, device(dz, 0, dc))
    for dy in range(1, 4):
        signal(barrier, device(0, dy))
    for k in range(2, PLANES):
        load(k)

    def hail(which, dz):
        for slot, d in ((0, dz), (1, PLANES - dz)):
            signal(here.at[which, slot], device(d, 0))

    def heard(which, slots):
        for slot in range(slots):
            pl.semaphore_wait(here.at[which, slot], 1)

    def transpose(k):
        pltpu.make_async_copy(raw.at[k], raw.at[k], load_sem.at[k]).wait()
        for a in range(2):
            for start in range(0, chunk, LANES):
                tile = raw[k, a, :, start : start + LANES].T
                spot = plane(k) * PER + start // block
                turned[pl.ds(spot, LANES // block), a] = tile.reshape(LANES // block, block, rows)

    def send(i, turn, wanted=None):
        zt = (z + ORDER[i]) % PLANES
        yt = (y + along(i, turn, c)) % 4
        target = zt * PER + yt * 2 + (c + turn) % 2

        def go():
            pltpu.make_async_remote_copy(
                src_ref=turned.at[target],
                dst_ref=got.at[me],
                send_sem=send_sem,
                recv_sem=recv_sem.at[turn],
                device_id={"batch": target},
                device_id_type=MESH,
            ).start()

        ok = wanted(zt, yt) if wanted else None
        if ORDER[i] == 0:
            ok = target != me if ok is None else ok & (target != me)
        if ok is None:
            go()
        else:
            pl.when(ok)(go)

    def urgency(level):
        def wanted(zt, yt):
            first = jnp.minimum(z, zt)
            return first >= level if level == EARLY else first == level

        return wanted

    def push(mask, r0, r1):
        groups = {"N": NEAR, "T": TWO, "F": [d for d in ORDER if d not in NEAR], "G": [d for d in ORDER if d not in NEAR + TWO]}
        which = [i for i in range(PLANES) if ORDER[i] in groups.get(mask, ORDER)]

        def one(turn, carry):
            for i in which:
                send(i, turn, urgency(int(mask)) if mask.isdigit() else None)
            return carry

        if r1 - r0 <= 2 and mask in "NT":
            for turn in range(r0, r1):
                one(turn, 0)
        else:
            lax.fori_loop(r0, r1, one, 0)

    def pair(dz):
        for turn in range(2):
            send(ORDER.index(dz), turn)

    transpose(0)
    pl.semaphore_wait(barrier, 7)
    for dy in range(1, 4):
        signal(here.at[0, dy - 1], device(0, dy))
    pair(1)
    transpose(1)
    pair(PLANES - 1)
    for k in range(2, 4):
        transpose(k)
    heard(0, 3)
    hail(1, 1)
    push("N", 2, FIRST)
    for k in range(4, 6):
        transpose(k)
    heard(1, 2)
    hail(2, 2)
    push("T", 0, SECOND)
    for k in range(6, PLANES):
        transpose(k)
    heard(2, 2)
    for mask, r0, r1 in PHASES:
        push(mask, r0, r1)

    got[me] = turned[me]

    def arrived(count, turn):
        pieces = pl.ds(0, count)
        pltpu.make_async_remote_copy(
            src_ref=turned.at[pieces],
            dst_ref=got.at[pieces],
            send_sem=send_sem,
            recv_sem=recv_sem.at[turn],
            device_id={"batch": (me + 1) % n},
            device_id_type=MESH,
        ).wait_recv()

    def take(turn, sums):
        own = turn == (8 - SHIFT[OWN] - 2 * c) % 4 * 2

        @pl.when(own)
        def _():
            arrived(PLANES - 1, turn)

        @pl.when(jnp.logical_not(own))
        def _():
            arrived(PLANES, turn)

        for i in range(PLANES):
            cs = (c + turn) % 2
            ys = (y - along(i, turn, cs) + 4) % 4
            source = (z - ORDER[i] + PLANES) % PLANES * PER + ys * 2 + cs
            out = []
            for a in range(2):
                low, high = sums[a]
                values = got[source, a]
                for start in range(0, rows, LANES):
                    part = values[:, start : start + LANES]
                    low += jnp.minimum(part, 1.0)
                    high += jnp.maximum(part, 1.0)
                out.append((low, high))
            sums = tuple(out)
        return sums

    zero = jnp.zeros((block, LANES), jnp.float32)
    sums = lax.fori_loop(0, PER, take, ((zero, zero), (zero, zero)))
    for a in range(2):
        for kind in range(2):
            total[a, kind] = sums[a][kind]

    others = pl.ds(0, n - 1)
    pltpu.make_async_remote_copy(
        src_ref=turned.at[others],
        dst_ref=got.at[others],
        send_sem=send_sem,
        recv_sem=recv_sem.at[0],
        device_id={"batch": (me + 1) % n},
        device_id_type=MESH,
    ).wait_send()


def rescale(got, total, first_out, second_out, ready, store_sem):
    n, _, block, rows = got.shape
    outs = (first_out, second_out)
    pieces = 4
    each = n // pieces
    copies = []
    for a in range(2):
        low, high = (
            jnp.sum(total[a, kind], axis=1, keepdims=True) / (n * rows) for kind in range(2)
        )
        scale = 1.0 / (high - low + 0.1)
        low = jnp.broadcast_to(low, (block, rows))
        scale = jnp.broadcast_to(scale, (block, rows))
        for piece in range(pieces):

            def turn(step, carry, a=a, piece=piece, low=low, scale=scale):
                source = piece * each + step
                start = pl.multiple_of(source * rows, LANES)
                ready[a, :, pl.ds(start, rows)] = (got[source, a] - low) * scale
                return carry

            lax.fori_loop(0, each, turn, 0, unroll=4)
            part = pl.ds(piece * each * rows, each * rows)
            copy = pltpu.make_async_copy(
                ready.at[a, :, part], outs[a].at[:, part], store_sem.at[a, piece]
            )
            copy.start()
            copies.append(copy)
    for copy in copies:
        copy.wait()


def solution(mesh):
    n = mesh.shape["batch"]

    def shards(samples_in, second_samples_in):
        rows, width = samples_in.shape
        block = width // n
        held = 2 * rows * width * 4
        got, total = pl.pallas_call(
            kernel,
            out_shape=(
                pltpu.VMEM((n, 2, block, rows), jnp.float32),
                pltpu.VMEM((2, 2, block, LANES), jnp.float32),
            ),
            in_specs=[pl.BlockSpec(memory_space=pltpu.HBM)] * 2,
            out_specs=[pl.BlockSpec(memory_space=pltpu.VMEM)] * 2,
            scratch_shapes=[
                pltpu.VMEM((PLANES, 2, rows, PER * block), jnp.float32),
                pltpu.VMEM((n, 2, block, rows), jnp.float32),
                pltpu.SemaphoreType.DMA((PLANES,)),
                pltpu.SemaphoreType.DMA,
                pltpu.SemaphoreType.DMA((PER,)),
                pltpu.SemaphoreType.REGULAR((3, 3)),
            ],
            compiler_params=pltpu.CompilerParams(
                collective_id=0, has_side_effects=True, vmem_limit_bytes=4 * held + (8 << 20)
            ),
            name="exchange",
        )(
            pltpu.with_memory_space_constraint(samples_in, pltpu.HBM),
            pltpu.with_memory_space_constraint(second_samples_in, pltpu.HBM),
        )
        out = jax.ShapeDtypeStruct((block, n * rows), jnp.float32)
        first, second = pl.pallas_call(
            rescale,
            out_shape=(out, out),
            in_specs=[pl.BlockSpec(memory_space=pltpu.VMEM)] * 2,
            out_specs=[pl.BlockSpec(memory_space=pl.ANY)] * 2,
            scratch_shapes=[
                pltpu.VMEM((2, block, n * rows), jnp.float32),
                pltpu.SemaphoreType.DMA((2, 4)),
            ],
            compiler_params=pltpu.CompilerParams(vmem_limit_bytes=2 * held + (8 << 20)),
            name="rescale",
        )(
            pltpu.with_memory_space_constraint(got, pltpu.VMEM),
            pltpu.with_memory_space_constraint(total, pltpu.VMEM),
        )
        return first.T, second.T

    placed = (P("batch", "group"), P("batch", "group"))
    return jax.shard_map(
        shards,
        mesh=mesh,
        in_specs=placed,
        out_specs=(P(None, ("group", "batch")), P(None, ("group", "batch"))),
        check_vma=False,
    )
```
